32 devices in a mesh: mem: 4 (over y, x), tile: 8 (over z, core).
Axes of the slice: x: 2, y: 2, z: 4, core: 2. Of those that a mesh axis runs over, the one named last changes fastest.
Arguments:
- ensemble: bfloat16 [8, 256, 64, 256], P('mem', None, 'tile'), may hold values from -4 to 4
- control: float32 [8, 64, 256], P('mem', 'tile'), may hold values from -6 to 6
- weights: float32 [8], P('mem'), may hold values from 0.1 to 0.6
- member_band: int32 [8], P('mem'), may hold values from 0 to 3
- spread: float32 [4], replicated, may hold values from 0.05 to 0.24
- advect: float32 [2, 256], replicated, may hold values from -0.9 to 0.9
- damping: float32 [256], replicated, may hold values from 0.02 to 0.2
- innovation: float32 [256, 64, 256], P(None, 'tile'), may hold values from -4 to 4
- obs_weight: float32 [64, 256], P('tile'), may hold values from 0.3 to 27
Outputs:
- grad_control: float32 [8, 64, 256], P('mem', 'tile')
- grad_weight: float32 [8], P('mem')
The draws below stay inside these ranges and needn't reach their ends.
All inputs are finite; a program needn't handle non-finite values.
Results may differ from the reference program's by a relative error of at most 0.0003.
Values sent between devices are 32-bit elements; how exact they have to be, the bound alone decides.
A program may use at most 64 MiB of HBM per device.

```python
import math
import jax
import jax.numpy as jnp
from jax import lax

VL = 256
NY = 256
SWEEPS = 8
BANDS = 4
M = 8
NX = 64


def draw_obs_weight(key, part):
    position = jnp.arange(NX, dtype=jnp.float32) / max(NX - 1, 1)
    ramp = jnp.exp(jnp.log(3.0) * position)
    noise = jax.random.uniform(key, (NX, NY), jnp.float32, 0.5, 2.0)
    return ramp[:, None] * noise


def touch_ends(drawn, stream_key, low, high):
    index_at = [jax.random.randint(jax.random.fold_in(stream_key, axis), (), 0, length) for axis, length in enumerate(drawn.shape)]
    longest = drawn.shape.index(max(drawn.shape))
    beside = index_at[:longest] + [(index_at[longest] + 1) % drawn.shape[longest]] + index_at[longest + 1:]
    return drawn.at[tuple(index_at)].set(low).at[tuple(beside)].set(high)


def levels(rng, dims, shards, smallest, largest):
    level, own = 1.0, jax.random.fold_in(rng, 6)
    for dim, shards_of in shards:
        steps = jnp.exp(jax.random.uniform(jax.random.fold_in(own, dim), (shards_of,), jnp.float32, smallest / len(shards), largest / len(shards)))
        level = level * jnp.repeat(steps, dims[dim] // shards_of).reshape([-1 if axis == dim else 1 for axis in range(len(dims))])
    return level


def bell_draw(own_key, shape, deviation, limit, shards=(), kind=jnp.bfloat16):
    drawn = jax.random.normal(own_key, shape, jnp.float32) * deviation
    if len(shards) > 0:
        drawn = levels(own_key, shape, shards, -0.22, 0.18) * drawn
    return jnp.clip(drawn, min=-limit, max=limit).astype(kind)


def setup_inputs(seed: int = 0) -> dict:
    seeds = jax.random.split(jax.random.key(seed), 10)
    return {
        "ensemble": bell_draw(seeds[0], (M, VL, NX, NY), 0.5, 4.0, ((0, 4), (2, 8))),
        "control": bell_draw(seeds[1], (M, NX, NY), 1.0, 6.0, ((0, 4), (1, 8)), jnp.float32),
        "weights": jnp.clip(0.1 + 0.5 * jax.random.uniform(seeds[2], (M,), jnp.float32) ** levels(seeds[2], (M,), ((0, 4),), -0.2, 0.2), 0.1, 0.6),
        "member_band": touch_ends(jax.random.randint(seeds[3], (M,), 0, BANDS), jax.random.fold_in(seeds[3], 1), 0, BANDS - 1).astype(jnp.int32),
        "spread": jnp.clip(jax.random.uniform(seeds[4], (BANDS,), jnp.float32, 0.05, 0.24), 0.05, 0.24),
        "advect": jnp.clip(jax.random.uniform(seeds[5], (2, VL), jnp.float32, -0.9, 0.9), -0.9, 0.9),
        "damping": jnp.clip(jax.random.uniform(seeds[6], (VL,), jnp.float32, 0.02, 0.2), 0.02, 0.2),
        "innovation": bell_draw(seeds[7], (VL, NX, NY), 0.5, 4.0, ((1, 8),), jnp.float32),
        "obs_weight": draw_obs_weight(jax.random.fold_in(seeds[9], 71), 0),
    }


def y_pairs(field):
    zero_col = jnp.zeros(field.shape[:-1] + (1,), field.dtype)
    north = jnp.concatenate([field[..., 1:], zero_col], axis=-1)
    south = jnp.concatenate([zero_col, field[..., :-1]], axis=-1)
    return (north, south)

def laplace(field):
    north, south = y_pairs(field)
    return jnp.roll(field, -1, -2) + jnp.roll(field, 1, -2) + north + south - 4.0 * field

def localize(field, rates):
    for sweep in range(SWEEPS):
        field = field + rates * laplace(field)
    return field

def dynamics(field, along_x, along_y, smooth):
    east = jnp.roll(field, -1, -2)
    west = jnp.roll(field, 1, -2)
    north, south = y_pairs(field)
    return field - along_x * ((east - west) * 0.5) - along_y * ((north - south) * 0.5) + smooth * (east + west + north + south - 4.0 * field)

def reference(ensemble, control, weights, member_band, spread, advect, damping, innovation, obs_weight):
    one_hot = (member_band[:, None] == jnp.arange(spread.shape[0], dtype=jnp.int32)[None, :]).astype(spread.dtype)
    rates = jnp.dot(one_hot, spread, precision=lax.Precision.HIGHEST)[:, None, None]
    localized = localize(control, rates)

    def accumulate(total, pair):
        member, field = pair
        return (total + member.astype(control.dtype) * field[None], None)
    scaled = weights[:, None, None] * localized
    increment, unused = lax.scan(accumulate, jnp.zeros(ensemble.shape[1:], control.dtype), (ensemble, scaled))
    along_x = advect[0][:, None, None]
    along_y = advect[1][:, None, None]
    smooth = damping[:, None, None]
    forward = dynamics(increment, along_x, along_y, smooth)
    weighted = obs_weight[None] * (forward - innovation)
    gradient = dynamics(weighted, -along_x, -along_y, smooth)

    def project(member):
        return lax.optimization_barrier(jnp.sum(member.astype(control.dtype) * gradient, axis=0))
    projected = lax.map(project, ensemble)
    grad_control = control + localize(weights[:, None, None] * projected, rates)
    grad_weight = lax.optimization_barrier(jnp.sum(localized * projected, axis=(1, 2))) / math.sqrt(NX * NY * VL)
    return (grad_control, grad_weight)
```

```python
import functools
import math

import jax
import jax.numpy as jnp
from jax import lax
from jax.experimental import pallas as pl
from jax.experimental.pallas import tpu as pltpu
from jax.sharding import PartitionSpec as P

SWEEPS = 8
STEPS = 8
LAG_C = 2
LAG_D = 4
LAG_E = 6
LAG_F = 7
MESH = pl.DeviceIdType.MESH


def factors(n):
    a = max(d for d in range(1, n + 1) if n % d == 0 and d * d <= n)
    return a, n // a


def y_pair(f):
    ny = f.shape[-1]
    col = lax.broadcasted_iota(jnp.int32, f.shape, 1)
    north = jnp.where(col == ny - 1, 0.0, pltpu.roll(f, ny - 1, 1))
    south = jnp.where(col == 0, 0.0, pltpu.roll(f, 1, 1))
    return north, south


def stencil(f, a, b, e):
    rows = f.shape[0]
    north, south = y_pair(f)
    east = pltpu.roll(f, rows - 1, 0)
    west = pltpu.roll(f, 1, 0)
    return (
        (1.0 - 4.0 * e) * f
        + (e - 0.5 * a) * east
        + (e + 0.5 * a) * west
        + (e - 0.5 * b) * north
        + (e + 0.5 * b) * south
    )


def sweeps(f, rates):
    rows = f.shape[0]
    for _ in range(SWEEPS):
        north, south = y_pair(f)
        east = pltpu.roll(f, rows - 1, 0)
        west = pltpu.roll(f, 1, 0)
        f = f + rates * (east + west + north + south - 4.0 * f)
    return f


def kernel(
    n, tiles, steps, planes,
    ens, control, weights, band, spread, advect, damping, innov, obs,
    out, gw_out,
    e_v, iv, loc, scl, proj, own, part, grad, r1a, r1b, r2a, r2b,
    ch, wh, ih, hh, ph, gwr,
    e_sem, i_sem,
    s1s, s1r, s2s, s2r, s3s, s3r, s4s, s4r,
    hs, hr, xs, xr, gs, gr,
):
    a, b = factors(n)
    ml = control.shape[0]
    rows = control.shape[1]
    me = lax.axis_index("mem")
    t = lax.axis_index("tile")
    ia = me // b
    ib = me % b
    nxt = (t + 1) % tiles
    prv = (t + tiles - 1) % tiles
    r1 = (r1a, r1b)
    r2 = (r2a, r2b)
    first = (b, a)
    second = (a, b)
    fi = (ib, ia)
    gi = (ia, ib)

    def device(q, f, g):
        return g * b + f if q == 0 else f * b + g

    def plane0(s, q):
        return (s * 2 + q) * (n * planes)

    def mine(q):
        return (fi[q] * second[q] + gi[q]) * planes

    for m in range(ml):
        pltpu.make_async_copy(ens.at[m], e_v.at[m], e_sem.at[m]).start()

    def innov_copy(s, q):
        return pltpu.make_async_copy(
            innov.at[pl.ds(plane0(s, q) + mine(q), planes)],
            iv.at[pl.ds((s * 2 + q) * planes, planes)],
            i_sem.at[s, q],
        )

    @pl.loop(0, steps)
    def _(s):
        for q in range(2):
            innov_copy(s, q).start()

    barrier = pltpu.get_barrier_semaphore()
    for d in range(1, tiles):
        pl.semaphore_signal(
            barrier, inc=1, device_id={"tile": (t + d) % tiles}, device_id_type=MESH
        )
    for d in range(1, b):
        pl.semaphore_signal(
            barrier, inc=1, device_id={"mem": device(0, (ib + d) % b, ia)}, device_id_type=MESH
        )
    for d in range(1, a):
        pl.semaphore_signal(
            barrier, inc=1, device_id={"mem": device(0, ib, (ia + d) % a)}, device_id_type=MESH
        )
    pl.semaphore_wait(barrier, tiles - 1 + a - 1 + b - 1)

    def to_tile(src, dst, k, dev):
        return pltpu.make_async_remote_copy(
            src_ref=src, dst_ref=dst, send_sem=xs.at[k], recv_sem=xr.at[k],
            device_id={"tile": dev}, device_id_type=MESH,
        )

    def both(src, dst, k):
        return (
            to_tile(src, dst.at[0], k, nxt),
            to_tile(src, dst.at[1], k + 1, prv),
        )

    c_copy = both(control, ch, 0)
    w_copy = both(obs, wh, 2)
    i_copy = both(iv, ih, 4)
    p_copy = both(scl, ph, 6)
    for c in c_copy + w_copy:
        c.start()

    rate_rows = []
    for m in range(ml):
        rate_rows.append(
            jnp.full((3 * rows, control.shape[2]), spread[band[m]], jnp.float32)
        )
    rates = jnp.concatenate(rate_rows, axis=0)
    for c in c_copy:
        c.wait_recv()
    field = []
    for m in range(ml):
        field += [ch[0, m], control[m], ch[1, m]]
    field = sweeps(jnp.concatenate(field, axis=0), rates)
    for m in range(ml):
        center = field[(3 * m + 1) * rows : (3 * m + 2) * rows]
        loc[m] = center
        scl[m] = weights[m] * center
        proj[m] = jnp.zeros_like(center)
    for m in range(ml):
        pltpu.make_async_copy(ens.at[m], e_v.at[m], e_sem.at[m]).wait()

    def stage1(s, q, d):
        f, g = first[q], second[q]
        to = (fi[q] + d) % f
        return pltpu.make_async_remote_copy(
            src_ref=part.at[s, q, pl.ds(to * (g * planes), g * planes)],
            dst_ref=r1[q].at[s, d - 1],
            send_sem=s1s.at[s, q, d - 1], recv_sem=s1r.at[s, q, d - 1],
            device_id={"mem": device(q, to, gi[q])}, device_id_type=MESH,
        )

    def stage2(s, q, d):
        g = second[q]
        to = (gi[q] + d) % g
        return pltpu.make_async_remote_copy(
            src_ref=part.at[s, q, pl.ds((fi[q] * g + to) * planes, planes)],
            dst_ref=r2[q].at[s, d - 1],
            send_sem=s2s.at[s, q, d - 1], recv_sem=s2r.at[s, q, d - 1],
            device_id={"mem": device(q, fi[q], to)}, device_id_type=MESH,
        )

    def stage3(s, q, d, incoming=False):
        g = second[q]
        to = (gi[q] + d) % g
        where = (gi[q] + g - d) % g if incoming else gi[q]
        block = grad.at[s, q, pl.ds((fi[q] * g + where) * planes, planes)]
        return pltpu.make_async_remote_copy(
            src_ref=block, dst_ref=block,
            send_sem=s3s.at[s, q, d - 1], recv_sem=s3r.at[s, q, d - 1],
            device_id={"mem": device(q, fi[q], to)}, device_id_type=MESH,
        )

    def stage4(s, q, d, incoming=False):
        f, g = first[q], second[q]
        to = (fi[q] + d) % f
        where = (fi[q] + f - d) % f if incoming else fi[q]
        block = grad.at[s, q, pl.ds(where * (g * planes), g * planes)]
        return pltpu.make_async_remote_copy(
            src_ref=block, dst_ref=block,
            send_sem=s4s.at[s, q, d - 1], recv_sem=s4r.at[s, q, d - 1],
            device_id={"mem": device(q, to, gi[q])}, device_id_type=MESH,
        )

    def halo(s):
        return tuple(
            pltpu.make_async_remote_copy(
                src_ref=own.at[s], dst_ref=hh.at[way, s],
                send_sem=hs.at[way, s], recv_sem=hr.at[way, s],
                device_id={"tile": dev}, device_id_type=MESH,
            )
            for way, dev in enumerate((nxt, prv))
        )

    def part_of(s):
        for q in range(2):
            total = None
            for m in range(ml):
                term = e_v[m, pl.ds(plane0(s, q), n * planes)].astype(jnp.float32) * scl[m][None]
                total = term if total is None else total + term
            part[s, q] = total
        for q in range(2):
            for d in range(1, first[q]):
                stage1(s, q, d).start()

    def reduce_first(s):
        for q in range(2):
            g = second[q]
            for d in range(1, first[q]):
                stage1(s, q, d).wait_recv()
            block = pl.ds(fi[q] * (g * planes), g * planes)
            total = part[s, q, block]
            for d in range(1, first[q]):
                total = total + r1[q][s, d - 1]
            part[s, q, block] = total
        for q in range(2):
            for d in range(1, second[q]):
                stage2(s, q, d).start()

    def reduce_second(s):
        for q in range(2):
            for d in range(1, second[q]):
                stage2(s, q, d).wait_recv()
            total = part[s, q, pl.ds(mine(q), planes)]
            for d in range(1, second[q]):
                total = total + r2[q][s, d - 1]
            own[s, q * planes : (q + 1) * planes] = total
        for c in halo(s):
            c.start()

    def adjoint(s):
        for c in halo(s):
            c.wait_recv()
        weight = jnp.concatenate([wh[0], obs[...], wh[1]], axis=0)
        for q in range(2):
            for p in range(planes):
                k = plane0(s, q) + mine(q) + p
                ax = advect[0, k]
                ay = advect[1, k]
                e = damping[k]
                i = q * planes + p
                j = s * (2 * planes) + i
                f = jnp.concatenate([hh[0, s, i], own[s, i], hh[1, s, i]], axis=0)
                o = jnp.concatenate([ih[0, j], iv[j], ih[1, j]], axis=0)
                w = weight * (stencil(f, ax, ay, e) - o)
                grad[s, q, mine(q) + p] = stencil(w, -ax, -ay, e)[rows : 2 * rows]
        for q in range(2):
            for d in range(1, second[q]):
                stage3(s, q, d).start()

    def spread_grad(s):
        for q in range(2):
            for d in range(1, second[q]):
                stage3(s, q, d, True).wait_recv()
        for q in range(2):
            for d in range(1, first[q]):
                stage4(s, q, d).start()

    def project(s):
        for q in range(2):
            for d in range(1, first[q]):
                stage4(s, q, d, True).wait_recv()
        for q in range(2):
            g = grad[s, q]
            for m in range(ml):
                e = e_v[m, pl.ds(plane0(s, q), n * planes)].astype(jnp.float32)
                proj[m] += jnp.sum(e * g, axis=0)

    @pl.loop(0, steps)
    def _(s):
        part_of(s)

    @pl.loop(0, steps)
    def _(s):
        for q in range(2):
            innov_copy(s, q).wait()

    for c in i_copy:
        c.start()
    for c in w_copy + i_copy:
        c.wait_recv()

    @pl.loop(0, steps + LAG_F)
    def _(tick):
        for lag, stage in (
            (0, reduce_first),
            (LAG_C, reduce_second),
            (LAG_D, adjoint),
            (LAG_E, spread_grad),
            (LAG_F, project),
        ):
            @pl.when(jnp.logical_and(tick >= lag, tick < steps + lag))
            def _(lag=lag, stage=stage):
                stage(tick - lag)

    for m in range(ml):
        scl[m] = weights[m] * proj[m]
    row = lax.broadcasted_iota(jnp.int32, (8, 128), 0)
    sums = jnp.zeros((8, 128), jnp.float32)
    for m in range(ml):
        v = jnp.sum(loc[m] * proj[m], axis=0, keepdims=True)
        v = sum(v[:, c : c + 128] for c in range(0, v.shape[1], 128))
        sums = jnp.where(row == m, jnp.broadcast_to(v, (8, 128)), sums)
    gwr[t] = sums
    for c in p_copy:
        c.start()

    def gw_copy(d, incoming=False):
        slot = (t + tiles - d) % tiles if incoming else t
        return pltpu.make_async_remote_copy(
            src_ref=gwr.at[slot], dst_ref=gwr.at[slot],
            send_sem=gs.at[d - 1], recv_sem=gr.at[d - 1],
            device_id={"tile": (t + d) % tiles}, device_id_type=MESH,
        )

    for d in range(1, tiles):
        gw_copy(d).start()
    for c in p_copy:
        c.wait_recv()
    field = []
    for m in range(ml):
        field += [ph[0, m], scl[m], ph[1, m]]
    field = sweeps(jnp.concatenate(field, axis=0), rates)
    for m in range(ml):
        out[m] = control[m] + field[(3 * m + 1) * rows : (3 * m + 2) * rows]
    for d in range(1, tiles):
        gw_copy(d, True).wait_recv()
    total = gwr[0]
    for d in range(1, tiles):
        total = total + gwr[d]
    gw_out[...] = jnp.broadcast_to(jnp.sum(total, axis=1, keepdims=True), (8, 128))

    for c in c_copy + w_copy + i_copy + p_copy:
        c.wait_send()
    for d in range(1, tiles):
        gw_copy(d).wait_send()

    @pl.loop(0, steps)
    def _(s):
        for c in halo(s):
            c.wait_send()
        for q in range(2):
            for d in range(1, first[q]):
                stage1(s, q, d).wait_send()
                stage4(s, q, d).wait_send()
            for d in range(1, second[q]):
                stage2(s, q, d).wait_send()
                stage3(s, q, d).wait_send()


def per_device(
    n, tiles,
    ensemble, control, weights, member_band, spread, advect, damping, innovation, obs_weight
):
    ml, vl, rows, ny = ensemble.shape
    assert rows == SWEEPS and ny % 128 == 0 and ml <= 8 and vl % (2 * n) == 0
    steps = max(d for d in range(1, STEPS + 1) if (vl // (2 * n)) % d == 0)
    planes = vl // (2 * n * steps)
    a, b = factors(n)
    f32 = jnp.float32
    peers = max(a, b, 2) - 1
    dma = pltpu.SemaphoreType.DMA
    vmem = pl.BlockSpec(memory_space=pltpu.VMEM)
    smem = pl.BlockSpec(memory_space=pltpu.SMEM)
    hbm = pl.BlockSpec(memory_space=pl.ANY)
    field = (rows, ny)
    out, gw = pl.pallas_call(
        functools.partial(kernel, n, tiles, steps, planes),
        out_shape=(
            jax.ShapeDtypeStruct((ml, rows, ny), f32),
            jax.ShapeDtypeStruct((8, 128), f32),
        ),
        in_specs=[hbm, vmem, smem, smem, smem, smem, smem, hbm, vmem],
        out_specs=(vmem, vmem),
        scratch_shapes=[
            pltpu.VMEM((ml, vl) + field, ensemble.dtype),
            pltpu.VMEM((steps * 2 * planes,) + field, f32),
            pltpu.VMEM((ml,) + field, f32),
            pltpu.VMEM((ml,) + field, f32),
            pltpu.VMEM((ml,) + field, f32),
            pltpu.VMEM((steps, 2 * planes) + field, f32),
            pltpu.VMEM((steps, 2, n * planes) + field, f32),
            pltpu.VMEM((steps, 2, n * planes) + field, f32),
            pltpu.VMEM((steps, max(b - 1, 1), a * planes) + field, f32),
            pltpu.VMEM((steps, max(a - 1, 1), b * planes) + field, f32),
            pltpu.VMEM((steps, max(a - 1, 1), planes) + field, f32),
            pltpu.VMEM((steps, max(b - 1, 1), planes) + field, f32),
            pltpu.VMEM((2, ml) + field, f32),
            pltpu.VMEM((2,) + field, f32),
            pltpu.VMEM((2, steps * 2 * planes) + field, f32),
            pltpu.VMEM((2, steps, 2 * planes) + field, f32),
            pltpu.VMEM((2, ml) + field, f32),
            pltpu.VMEM((tiles, 8, 128), f32),
            dma((ml,)),
            dma((steps, 2)),
        ]
        + [dma((steps, 2, peers))] * 8
        + [dma((2, steps))] * 2
        + [dma((8,))] * 2
        + [dma((tiles - 1,))] * 2,
        compiler_params=pltpu.CompilerParams(
            collective_id=0, has_side_effects=True, vmem_limit_bytes=60 * 1024 * 1024
        ),
    )(ensemble, control, weights, member_band, spread, advect, damping, innovation, obs_weight)
    total_cells = tiles * rows * ny * vl
    return out, gw[:ml, 0] / math.sqrt(total_cells)


def solution(mesh):
    in_specs = (
        P("mem", None, "tile", None),
        P("mem", "tile", None),
        P("mem"),
        P("mem"),
        P(),
        P(),
        P(),
        P(None, "tile", None),
        P("tile", None),
    )
    out_specs = (P("mem", "tile", None), P("mem"))
    return jax.shard_map(
        functools.partial(per_device, mesh.shape["mem"], mesh.shape["tile"]),
        mesh=mesh, in_specs=in_specs, out_specs=out_specs, check_vma=False,
    )
```

```python
import functools
import math

import jax
import jax.numpy as jnp
from jax import lax
from jax.experimental import pallas as pl
from jax.experimental.pallas import tpu as pltpu
from jax.sharding import PartitionSpec as P

SWEEPS = 8
STEPS = 8
LAG_C = 2
LAG_D = 4
LAG_E = 6
LAG_F = 7
MESH = pl.DeviceIdType.MESH


def factors(n):
    a = max(d for d in range(1, n + 1) if n % d == 0 and d * d <= n)
    return a, n // a


def y_pair(f):
    ny = f.shape[-1]
    col = lax.broadcasted_iota(jnp.int32, f.shape, 1)
    north = jnp.where(col == ny - 1, 0.0, pltpu.roll(f, ny - 1, 1))
    south = jnp.where(col == 0, 0.0, pltpu.roll(f, 1, 1))
    return north, south


def stencil(f, a, b, e):
    rows = f.shape[0]
    north, south = y_pair(f)
    east = pltpu.roll(f, rows - 1, 0)
    west = pltpu.roll(f, 1, 0)
    return (
        (1.0 - 4.0 * e) * f
        + (e - 0.5 * a) * east
        + (e + 0.5 * a) * west
        + (e - 0.5 * b) * north
        + (e + 0.5 * b) * south
    )


def sweeps(f, rates):
    rows = f.shape[0]
    for _ in range(SWEEPS):
        north, south = y_pair(f)
        east = pltpu.roll(f, rows - 1, 0)
        west = pltpu.roll(f, 1, 0)
        f = f + rates * (east + west + north + south - 4.0 * f)
    return f


def kernel(
    n, tiles, steps, planes,
    ens, control, weights, band, spread, advect, damping, innov, obs,
    out, gw_out,
    e_v, iv, loc, scl, proj, own, part, grad, r1a, r1b, r2a, r2b,
    ch, wh, ih, hh, ph, gwr,
    e_sem, i_sem,
    s1s, s1r, s2s, s2r, s3s, s3r, s4s, s4r,
    hs, hr, xs, xr, gs, gr,
):
    a, b = factors(n)
    ml = control.shape[0]
    rows = control.shape[1]
    me = lax.axis_index("mem")
    t = lax.axis_index("tile")
    ia = me // b
    ib = me % b
    nxt = (t + 1) % tiles
    prv = (t + tiles - 1) % tiles
    r1 = (r1a, r1b)
    r2 = (r2a, r2b)
    first = (b, a)
    second = (a, b)
    fi = (ib, ia)
    gi = (ia, ib)

    def device(q, f, g):
        return g * b + f if q == 0 else f * b + g

    def plane0(s, q):
        return (s * 2 + q) * (n * planes)

    def mine(q):
        return (fi[q] * second[q] + gi[q]) * planes

    for m in range(ml):
        pltpu.make_async_copy(ens.at[m], e_v.at[m], e_sem.at[m]).start()

    def innov_copy(s, q):
        return pltpu.make_async_copy(
            innov.at[pl.ds(plane0(s, q) + mine(q), planes)],
            iv.at[pl.ds((s * 2 + q) * planes, planes)],
            i_sem.at[s, q],
        )

    @pl.loop(0, steps)
    def _(s):
        for q in range(2):
            innov_copy(s, q).start()

    barrier = pltpu.get_barrier_semaphore()
    for d in range(1, tiles):
        pl.semaphore_signal(
            barrier, inc=1, device_id={"tile": (t + d) % tiles}, device_id_type=MESH
        )
    for d in range(1, b):
        pl.semaphore_signal(
            barrier, inc=1, device_id={"mem": device(0, (ib + d) % b, ia)}, device_id_type=MESH
        )
    for d in range(1, a):
        pl.semaphore_signal(
            barrier, inc=1, device_id={"mem": device(0, ib, (ia + d) % a)}, device_id_type=MESH
        )
    pl.semaphore_wait(barrier, tiles - 1 + a - 1 + b - 1)

    def to_tile(src, dst, k, dev):
        return pltpu.make_async_remote_copy(
            src_ref=src, dst_ref=dst, send_sem=xs.at[k], recv_sem=xr.at[k],
            device_id={"tile": dev}, device_id_type=MESH,
        )

    def both(src, dst, k):
        return (
            to_tile(src, dst.at[0], k, nxt),
            to_tile(src, dst.at[1], k + 1, prv),
        )

    c_copy = both(control, ch, 0)
    w_copy = both(obs, wh, 2)
    i_copy = (
        to_tile(iv.at[:, rows - 1 :, :], ih.at[0, :, rows - 1 :, :], 4, nxt),
        to_tile(iv.at[:, :1, :], ih.at[1, :, :1, :], 5, prv),
    )
    p_copy = both(scl, ph, 6)
    for c in c_copy + w_copy:
        c.start()

    @pl.loop(0, steps)
    def _(s):
        for q in range(2):
            innov_copy(s, q).wait()

    for c in i_copy:
        c.start()

    rate_rows = []
    for m in range(ml):
        rate_rows.append(
            jnp.full((3 * rows, control.shape[2]), spread[band[m]], jnp.float32)
        )
    rates = jnp.concatenate(rate_rows, axis=0)
    for c in c_copy:
        c.wait_recv()
    field = []
    for m in range(ml):
        field += [ch[0, m], control[m], ch[1, m]]
    field = sweeps(jnp.concatenate(field, axis=0), rates)
    for m in range(ml):
        center = field[(3 * m + 1) * rows : (3 * m + 2) * rows]
        loc[m] = center
        scl[m] = weights[m] * center
        proj[m] = jnp.zeros_like(center)
    for m in range(ml):
        pltpu.make_async_copy(ens.at[m], e_v.at[m], e_sem.at[m]).wait()

    def stage1(s, q, d):
        f, g = first[q], second[q]
        to = (fi[q] + d) % f
        return pltpu.make_async_remote_copy(
            src_ref=part.at[s, q, pl.ds(to * (g * planes), g * planes)],
            dst_ref=r1[q].at[s, d - 1],
            send_sem=s1s.at[s, q, d - 1], recv_sem=s1r.at[s, q, d - 1],
            device_id={"mem": device(q, to, gi[q])}, device_id_type=MESH,
        )

    def stage2(s, q, d):
        g = second[q]
        to = (gi[q] + d) % g
        return pltpu.make_async_remote_copy(
            src_ref=part.at[s, q, pl.ds((fi[q] * g + to) * planes, planes)],
            dst_ref=r2[q].at[s, d - 1],
            send_sem=s2s.at[s, q, d - 1], recv_sem=s2r.at[s, q, d - 1],
            device_id={"mem": device(q, fi[q], to)}, device_id_type=MESH,
        )

    def stage3(s, q, d, incoming=False):
        g = second[q]
        to = (gi[q] + d) % g
        where = (gi[q] + g - d) % g if incoming else gi[q]
        block = grad.at[s, q, pl.ds((fi[q] * g + where) * planes, planes)]
        return pltpu.make_async_remote_copy(
            src_ref=block, dst_ref=block,
            send_sem=s3s.at[s, q, d - 1], recv_sem=s3r.at[s, q, d - 1],
            device_id={"mem": device(q, fi[q], to)}, device_id_type=MESH,
        )

    def stage4(s, q, d, incoming=False):
        f, g = first[q], second[q]
        to = (fi[q] + d) % f
        where = (fi[q] + f - d) % f if incoming else fi[q]
        block = grad.at[s, q, pl.ds(where * (g * planes), g * planes)]
        return pltpu.make_async_remote_copy(
            src_ref=block, dst_ref=block,
            send_sem=s4s.at[s, q, d - 1], recv_sem=s4r.at[s, q, d - 1],
            device_id={"mem": device(q, to, gi[q])}, device_id_type=MESH,
        )

    def halo(s):
        return tuple(
            pltpu.make_async_remote_copy(
                src_ref=own.at[s, :, edge, :], dst_ref=hh.at[way, s, :, edge, :],
                send_sem=hs.at[way, s], recv_sem=hr.at[way, s],
                device_id={"tile": dev}, device_id_type=MESH,
            )
            for way, (dev, edge) in enumerate(
                ((nxt, slice(rows - 2, rows)), (prv, slice(0, 2)))
            )
        )

    def part_of(s):
        for q in range(2):
            total = None
            for m in range(ml):
                term = e_v[m, pl.ds(plane0(s, q), n * planes)].astype(jnp.float32) * scl[m][None]
                total = term if total is None else total + term
            part[s, q] = total
        for q in range(2):
            for d in range(1, first[q]):
                stage1(s, q, d).start()

    def reduce_first(s):
        for q in range(2):
            g = second[q]
            for d in range(1, first[q]):
                stage1(s, q, d).wait_recv()
            block = pl.ds(fi[q] * (g * planes), g * planes)
            total = part[s, q, block]
            for d in range(1, first[q]):
                total = total + r1[q][s, d - 1]
            part[s, q, block] = total
        for q in range(2):
            for d in range(1, second[q]):
                stage2(s, q, d).start()

    def reduce_second(s):
        for q in range(2):
            for d in range(1, second[q]):
                stage2(s, q, d).wait_recv()
            total = part[s, q, pl.ds(mine(q), planes)]
            for d in range(1, second[q]):
                total = total + r2[q][s, d - 1]
            own[s, q * planes : (q + 1) * planes] = total
        for c in halo(s):
            c.start()

    def adjoint(s):
        for c in halo(s):
            c.wait_recv()
        weight = jnp.concatenate([wh[0], obs[...], wh[1]], axis=0)
        for q in range(2):
            for p in range(planes):
                k = plane0(s, q) + mine(q) + p
                ax = advect[0, k]
                ay = advect[1, k]
                e = damping[k]
                i = q * planes + p
                j = s * (2 * planes) + i
                f = jnp.concatenate([hh[0, s, i], own[s, i], hh[1, s, i]], axis=0)
                o = jnp.concatenate([ih[0, j], iv[j], ih[1, j]], axis=0)
                w = weight * (stencil(f, ax, ay, e) - o)
                grad[s, q, mine(q) + p] = stencil(w, -ax, -ay, e)[rows : 2 * rows]
        for q in range(2):
            for d in range(1, second[q]):
                stage3(s, q, d).start()

    def spread_grad(s):
        for q in range(2):
            for d in range(1, second[q]):
                stage3(s, q, d, True).wait_recv()
        for q in range(2):
            for d in range(1, first[q]):
                stage4(s, q, d).start()

    def project(s):
        for q in range(2):
            for d in range(1, first[q]):
                stage4(s, q, d, True).wait_recv()
        for q in range(2):
            g = grad[s, q]
            for m in range(ml):
                e = e_v[m, pl.ds(plane0(s, q), n * planes)].astype(jnp.float32)
                proj[m] += jnp.sum(e * g, axis=0)

    @pl.loop(0, steps)
    def _(s):
        part_of(s)

    @pl.loop(0, steps + LAG_F)
    def _(tick):
        @pl.when(tick == LAG_D)
        def _():
            for c in w_copy + i_copy:
                c.wait_recv()

        for lag, stage in (
            (0, reduce_first),
            (LAG_C, reduce_second),
            (LAG_D, adjoint),
            (LAG_E, spread_grad),
            (LAG_F, project),
        ):
            @pl.when(jnp.logical_and(tick >= lag, tick < steps + lag))
            def _(lag=lag, stage=stage):
                stage(tick - lag)

    for m in range(ml):
        scl[m] = weights[m] * proj[m]
    row = lax.broadcasted_iota(jnp.int32, (8, 128), 0)
    sums = jnp.zeros((8, 128), jnp.float32)
    for m in range(ml):
        v = jnp.sum(loc[m] * proj[m], axis=0, keepdims=True)
        v = sum(v[:, c : c + 128] for c in range(0, v.shape[1], 128))
        sums = jnp.where(row == m, jnp.broadcast_to(v, (8, 128)), sums)
    gwr[t] = sums
    for c in p_copy:
        c.start()

    def gw_copy(d, incoming=False):
        slot = (t + tiles - d) % tiles if incoming else t
        return pltpu.make_async_remote_copy(
            src_ref=gwr.at[slot], dst_ref=gwr.at[slot],
            send_sem=gs.at[d - 1], recv_sem=gr.at[d - 1],
            device_id={"tile": (t + d) % tiles}, device_id_type=MESH,
        )

    for d in range(1, tiles):
        gw_copy(d).start()
    for c in p_copy:
        c.wait_recv()
    field = []
    for m in range(ml):
        field += [ph[0, m], scl[m], ph[1, m]]
    field = sweeps(jnp.concatenate(field, axis=0), rates)
    for m in range(ml):
        out[m] = control[m] + field[(3 * m + 1) * rows : (3 * m + 2) * rows]
    for d in range(1, tiles):
        gw_copy(d, True).wait_recv()
    total = gwr[0]
    for d in range(1, tiles):
        total = total + gwr[d]
    gw_out[...] = jnp.broadcast_to(jnp.sum(total, axis=1, keepdims=True), (8, 128))

    for c in c_copy + w_copy + i_copy + p_copy:
        c.wait_send()
    for d in range(1, tiles):
        gw_copy(d).wait_send()

    @pl.loop(0, steps)
    def _(s):
        for c in halo(s):
            c.wait_send()
        for q in range(2):
            for d in range(1, first[q]):
                stage1(s, q, d).wait_send()
                stage4(s, q, d).wait_send()
            for d in range(1, second[q]):
                stage2(s, q, d).wait_send()
                stage3(s, q, d).wait_send()


def per_device(
    n, tiles,
    ensemble, control, weights, member_band, spread, advect, damping, innovation, obs_weight
):
    ml, vl, rows, ny = ensemble.shape
    assert rows == SWEEPS and ny % 128 == 0 and ml <= 8 and vl % (2 * n) == 0
    steps = max(d for d in range(1, STEPS + 1) if (vl // (2 * n)) % d == 0)
    planes = vl // (2 * n * steps)
    a, b = factors(n)
    f32 = jnp.float32
    peers = max(a, b, 2) - 1
    dma = pltpu.SemaphoreType.DMA
    vmem = pl.BlockSpec(memory_space=pltpu.VMEM)
    smem = pl.BlockSpec(memory_space=pltpu.SMEM)
    hbm = pl.BlockSpec(memory_space=pl.ANY)
    field = (rows, ny)
    out, gw = pl.pallas_call(
        functools.partial(kernel, n, tiles, steps, planes),
        out_shape=(
            jax.ShapeDtypeStruct((ml, rows, ny), f32),
            jax.ShapeDtypeStruct((8, 128), f32),
        ),
        in_specs=[hbm, vmem, smem, smem, smem, smem, smem, hbm, vmem],
        out_specs=(vmem, vmem),
        scratch_shapes=[
            pltpu.VMEM((ml, vl) + field, ensemble.dtype),
            pltpu.VMEM((steps * 2 * planes,) + field, f32),
            pltpu.VMEM((ml,) + field, f32),
            pltpu.VMEM((ml,) + field, f32),
            pltpu.VMEM((ml,) + field, f32),
            pltpu.VMEM((steps, 2 * planes) + field, f32),
            pltpu.VMEM((steps, 2, n * planes) + field, f32),
            pltpu.VMEM((steps, 2, n * planes) + field, f32),
            pltpu.VMEM((steps, max(b - 1, 1), a * planes) + field, f32),
            pltpu.VMEM((steps, max(a - 1, 1), b * planes) + field, f32),
            pltpu.VMEM((steps, max(a - 1, 1), planes) + field, f32),
            pltpu.VMEM((steps, max(b - 1, 1), planes) + field, f32),
            pltpu.VMEM((2, ml) + field, f32),
            pltpu.VMEM((2,) + field, f32),
            pltpu.VMEM((2, steps * 2 * planes) + field, f32),
            pltpu.VMEM((2, steps, 2 * planes) + field, f32),
            pltpu.VMEM((2, ml) + field, f32),
            pltpu.VMEM((tiles, 8, 128), f32),
            dma((ml,)),
            dma((steps, 2)),
        ]
        + [dma((steps, 2, peers))] * 8
        + [dma((2, steps))] * 2
        + [dma((8,))] * 2
        + [dma((tiles - 1,))] * 2,
        compiler_params=pltpu.CompilerParams(
            collective_id=0, has_side_effects=True, vmem_limit_bytes=60 * 1024 * 1024
        ),
    )(ensemble, control, weights, member_band, spread, advect, damping, innovation, obs_weight)
    total_cells = tiles * rows * ny * vl
    return out, gw[:ml, 0] / math.sqrt(total_cells)


def solution(mesh):
    in_specs = (
        P("mem", None, "tile", None),
        P("mem", "tile", None),
        P("mem"),
        P("mem"),
        P(),
        P(),
        P(),
        P(None, "tile", None),
        P("tile", None),
    )
    out_specs = (P("mem", "tile", None), P("mem"))
    return jax.shard_map(
        functools.partial(per_device, mesh.shape["mem"], mesh.shape["tile"]),
        mesh=mesh, in_specs=in_specs, out_specs=out_specs, check_vma=False,
    )
```

```python
import functools
import math

import jax
import jax.numpy as jnp
from jax import lax
from jax.experimental import pallas as pl
from jax.experimental.pallas import tpu as pltpu
from jax.sharding import PartitionSpec as P

SWEEPS = 8
STEPS = 4
LAG_C = 2
LAG_D = 3
LAG_E = 4
LAG_F = 5
MESH = pl.DeviceIdType.MESH


def factors(n):
    a = max(d for d in range(1, n + 1) if n % d == 0 and d * d <= n)
    return a, n // a


def y_pair(f):
    ny = f.shape[-1]
    col = lax.broadcasted_iota(jnp.int32, f.shape, 1)
    north = jnp.where(col == ny - 1, 0.0, pltpu.roll(f, ny - 1, 1))
    south = jnp.where(col == 0, 0.0, pltpu.roll(f, 1, 1))
    return north, south


def stencil(f, a, b, e):
    rows = f.shape[0]
    north, south = y_pair(f)
    east = pltpu.roll(f, rows - 1, 0)
    west = pltpu.roll(f, 1, 0)
    return (
        (1.0 - 4.0 * e) * f
        + (e - 0.5 * a) * east
        + (e + 0.5 * a) * west
        + (e - 0.5 * b) * north
        + (e + 0.5 * b) * south
    )


def sweeps(f, rates):
    rows = f.shape[0]
    for _ in range(SWEEPS):
        north, south = y_pair(f)
        east = pltpu.roll(f, rows - 1, 0)
        west = pltpu.roll(f, 1, 0)
        f = f + rates * (east + west + north + south - 4.0 * f)
    return f


def kernel(
    n, tiles, steps, planes,
    ens, control_h, weights_h, band_h, spread_h, advect_h, damping_h, innov, obs_h,
    out_h, gw_h,
    control, weights, band, spread, advect, damping, obs, out, gw_out, arg_sem, out_sem,
    e_v, iv, loc, scl, proj, own, part, grad, r1a, r1b, r2a, r2b,
    ch, wh, ih, hh, ph, gwr,
    e_sem, i_sem,
    s1s, s1r, s2s, s2r, s3s, s3r, s4s, s4r,
    hs, hr, xs, xr, gs, gr,
):
    a, b = factors(n)
    ml = control.shape[0]
    rows = control.shape[1]
    me = lax.axis_index("mem")
    t = lax.axis_index("tile")
    ia = me // b
    ib = me % b
    nxt = (t + 1) % tiles
    prv = (t + tiles - 1) % tiles
    r1 = (r1a, r1b)
    r2 = (r2a, r2b)
    first = (b, a)
    second = (a, b)
    fi = (ib, ia)
    gi = (ia, ib)

    def device(q, f, g):
        return g * b + f if q == 0 else f * b + g

    def plane0(s, q):
        return (s * 2 + q) * (n * planes)

    def mine(q):
        return (fi[q] * second[q] + gi[q]) * planes

    args = [
        pltpu.make_async_copy(src, dst, arg_sem.at[i])
        for i, (src, dst) in enumerate((
            (control_h, control), (obs_h, obs), (weights_h, weights), (band_h, band),
            (spread_h, spread), (advect_h, advect), (damping_h, damping),
        ))
    ]
    for c in args:
        c.start()

    def innov_copy(s, q):
        return pltpu.make_async_copy(
            innov.at[pl.ds(plane0(s, q) + mine(q), planes)],
            iv.at[pl.ds((s * 2 + q) * planes, planes)],
            i_sem.at[s, q],
        )

    @pl.loop(0, steps)
    def _(s):
        for q in range(2):
            innov_copy(s, q).start()

    for m in range(ml):
        pltpu.make_async_copy(ens.at[m], e_v.at[m], e_sem.at[m]).start()

    barrier = pltpu.get_barrier_semaphore()
    for d in range(1, tiles):
        pl.semaphore_signal(
            barrier, inc=1, device_id={"tile": (t + d) % tiles}, device_id_type=MESH
        )
    for d in range(1, b):
        pl.semaphore_signal(
            barrier, inc=1, device_id={"mem": device(0, (ib + d) % b, ia)}, device_id_type=MESH
        )
    for d in range(1, a):
        pl.semaphore_signal(
            barrier, inc=1, device_id={"mem": device(0, ib, (ia + d) % a)}, device_id_type=MESH
        )
    pl.semaphore_wait(barrier, tiles - 1 + a - 1 + b - 1)

    def to_tile(src, dst, k, dev):
        return pltpu.make_async_remote_copy(
            src_ref=src, dst_ref=dst, send_sem=xs.at[k], recv_sem=xr.at[k],
            device_id={"tile": dev}, device_id_type=MESH,
        )

    def both(src, dst, k):
        return (
            to_tile(src, dst.at[0], k, nxt),
            to_tile(src, dst.at[1], k + 1, prv),
        )

    c_copy = both(control, ch, 0)
    w_copy = both(obs, wh, 2)
    i_copy = (
        to_tile(iv.at[:, rows - 1 :, :], ih.at[0, :, rows - 1 :, :], 4, nxt),
        to_tile(iv.at[:, :1, :], ih.at[1, :, :1, :], 5, prv),
    )
    p_copy = both(scl, ph, 6)
    for c in args[:2]:
        c.wait()
    for c in c_copy + w_copy:
        c.start()
    for c in args[2:]:
        c.wait()

    @pl.loop(0, steps)
    def _(s):
        for q in range(2):
            innov_copy(s, q).wait()

    for c in i_copy:
        c.start()

    rate_rows = []
    for m in range(ml):
        rate_rows.append(
            jnp.full((3 * rows, control.shape[2]), spread[band[m]], jnp.float32)
        )
    rates = jnp.concatenate(rate_rows, axis=0)
    for c in c_copy:
        c.wait_recv()
    field = []
    for m in range(ml):
        field += [ch[0, m], control[m], ch[1, m]]
    field = sweeps(jnp.concatenate(field, axis=0), rates)
    for m in range(ml):
        center = field[(3 * m + 1) * rows : (3 * m + 2) * rows]
        loc[m] = center
        scl[m] = weights[m] * center
        proj[m] = jnp.zeros_like(center)
    for m in range(ml):
        pltpu.make_async_copy(ens.at[m], e_v.at[m], e_sem.at[m]).wait()

    def stage1(s, q, d):
        f, g = first[q], second[q]
        to = (fi[q] + d) % f
        return pltpu.make_async_remote_copy(
            src_ref=part.at[s, q, pl.ds(to * (g * planes), g * planes)],
            dst_ref=r1[q].at[s, d - 1],
            send_sem=s1s.at[s, q, d - 1], recv_sem=s1r.at[s, q, d - 1],
            device_id={"mem": device(q, to, gi[q])}, device_id_type=MESH,
        )

    def stage2(s, q, d):
        g = second[q]
        to = (gi[q] + d) % g
        return pltpu.make_async_remote_copy(
            src_ref=part.at[s, q, pl.ds((fi[q] * g + to) * planes, planes)],
            dst_ref=r2[q].at[s, d - 1],
            send_sem=s2s.at[s, q, d - 1], recv_sem=s2r.at[s, q, d - 1],
            device_id={"mem": device(q, fi[q], to)}, device_id_type=MESH,
        )

    def stage3(s, q, d, incoming=False):
        g = second[q]
        to = (gi[q] + d) % g
        where = (gi[q] + g - d) % g if incoming else gi[q]
        block = grad.at[s, q, pl.ds((fi[q] * g + where) * planes, planes)]
        return pltpu.make_async_remote_copy(
            src_ref=block, dst_ref=block,
            send_sem=s3s.at[s, q, d - 1], recv_sem=s3r.at[s, q, d - 1],
            device_id={"mem": device(q, fi[q], to)}, device_id_type=MESH,
        )

    def stage4(s, q, d, incoming=False):
        f, g = first[q], second[q]
        to = (fi[q] + d) % f
        where = (fi[q] + f - d) % f if incoming else fi[q]
        block = grad.at[s, q, pl.ds(where * (g * planes), g * planes)]
        return pltpu.make_async_remote_copy(
            src_ref=block, dst_ref=block,
            send_sem=s4s.at[s, q, d - 1], recv_sem=s4r.at[s, q, d - 1],
            device_id={"mem": device(q, to, gi[q])}, device_id_type=MESH,
        )

    def halo(s):
        return tuple(
            pltpu.make_async_remote_copy(
                src_ref=own.at[s, :, edge, :], dst_ref=hh.at[way, s, :, edge, :],
                send_sem=hs.at[way, s], recv_sem=hr.at[way, s],
                device_id={"tile": dev}, device_id_type=MESH,
            )
            for way, (dev, edge) in enumerate(
                ((nxt, slice(rows - 2, rows)), (prv, slice(0, 2)))
            )
        )

    def part_of(s):
        for q in range(2):
            total = None
            for m in range(ml):
                term = e_v[m, pl.ds(plane0(s, q), n * planes)].astype(jnp.float32) * scl[m][None]
                total = term if total is None else total + term
            part[s, q] = total
        for q in range(2):
            for d in range(1, first[q]):
                stage1(s, q, d).start()

    def reduce_first(s):
        for q in range(2):
            g = second[q]
            for d in range(1, first[q]):
                stage1(s, q, d).wait_recv()
            block = pl.ds(fi[q] * (g * planes), g * planes)
            total = part[s, q, block]
            for d in range(1, first[q]):
                total = total + r1[q][s, d - 1]
            part[s, q, block] = total
        for q in range(2):
            for d in range(1, second[q]):
                stage2(s, q, d).start()

    def reduce_second(s):
        for q in range(2):
            for d in range(1, second[q]):
                stage2(s, q, d).wait_recv()
            total = part[s, q, pl.ds(mine(q), planes)]
            for d in range(1, second[q]):
                total = total + r2[q][s, d - 1]
            own[s, q * planes : (q + 1) * planes] = total
        for c in halo(s):
            c.start()

    def adjoint(s):
        for c in halo(s):
            c.wait_recv()
        weight = jnp.concatenate([wh[0], obs[...], wh[1]], axis=0)
        for q in range(2):
            for p in range(planes):
                k = plane0(s, q) + mine(q) + p
                ax = advect[0, k]
                ay = advect[1, k]
                e = damping[k]
                i = q * planes + p
                j = s * (2 * planes) + i
                f = jnp.concatenate([hh[0, s, i], own[s, i], hh[1, s, i]], axis=0)
                o = jnp.concatenate([ih[0, j], iv[j], ih[1, j]], axis=0)
                w = weight * (stencil(f, ax, ay, e) - o)
                grad[s, q, mine(q) + p] = stencil(w, -ax, -ay, e)[rows : 2 * rows]
        for q in range(2):
            for d in range(1, second[q]):
                stage3(s, q, d).start()

    def spread_grad(s):
        for q in range(2):
            for d in range(1, second[q]):
                stage3(s, q, d, True).wait_recv()
        for q in range(2):
            for d in range(1, first[q]):
                stage4(s, q, d).start()

    def project(s):
        for q in range(2):
            for d in range(1, first[q]):
                stage4(s, q, d, True).wait_recv()
        for q in range(2):
            g = grad[s, q]
            for m in range(ml):
                e = e_v[m, pl.ds(plane0(s, q), n * planes)].astype(jnp.float32)
                proj[m] += jnp.sum(e * g, axis=0)

    @pl.loop(0, steps)
    def _(s):
        part_of(s)

    @pl.loop(0, steps + LAG_F)
    def _(tick):
        @pl.when(tick == LAG_D)
        def _():
            for c in w_copy + i_copy:
                c.wait_recv()

        for lag, stage in (
            (0, reduce_first),
            (LAG_C, reduce_second),
            (LAG_D, adjoint),
            (LAG_E, spread_grad),
            (LAG_F, project),
        ):
            @pl.when(jnp.logical_and(tick >= lag, tick < steps + lag))
            def _(lag=lag, stage=stage):
                stage(tick - lag)

    for m in range(ml):
        scl[m] = weights[m] * proj[m]
    row = lax.broadcasted_iota(jnp.int32, (8, 128), 0)
    sums = jnp.zeros((8, 128), jnp.float32)
    for m in range(ml):
        v = jnp.sum(loc[m] * proj[m], axis=0, keepdims=True)
        v = sum(v[:, c : c + 128] for c in range(0, v.shape[1], 128))
        sums = jnp.where(row == m, jnp.broadcast_to(v, (8, 128)), sums)
    gwr[t] = sums
    for c in p_copy:
        c.start()

    def gw_copy(d, incoming=False):
        slot = (t + tiles - d) % tiles if incoming else t
        return pltpu.make_async_remote_copy(
            src_ref=gwr.at[slot], dst_ref=gwr.at[slot],
            send_sem=gs.at[d - 1], recv_sem=gr.at[d - 1],
            device_id={"tile": (t + d) % tiles}, device_id_type=MESH,
        )

    for d in range(1, tiles):
        gw_copy(d).start()
    for c in p_copy:
        c.wait_recv()
    field = []
    for m in range(ml):
        field += [ph[0, m], scl[m], ph[1, m]]
    field = sweeps(jnp.concatenate(field, axis=0), rates)
    for m in range(ml):
        out[m] = control[m] + field[(3 * m + 1) * rows : (3 * m + 2) * rows]
    outs = (
        pltpu.make_async_copy(out, out_h, out_sem.at[0]),
        pltpu.make_async_copy(gw_out, gw_h, out_sem.at[1]),
    )
    outs[0].start()
    for d in range(1, tiles):
        gw_copy(d, True).wait_recv()
    total = gwr[0]
    for d in range(1, tiles):
        total = total + gwr[d]
    gw_out[...] = jnp.broadcast_to(jnp.sum(total, axis=1, keepdims=True), (8, 128))
    outs[1].start()

    for c in c_copy + w_copy + i_copy + p_copy:
        c.wait_send()
    for d in range(1, tiles):
        gw_copy(d).wait_send()

    @pl.loop(0, steps)
    def _(s):
        for c in halo(s):
            c.wait_send()
        for q in range(2):
            for d in range(1, first[q]):
                stage1(s, q, d).wait_send()
                stage4(s, q, d).wait_send()
            for d in range(1, second[q]):
                stage2(s, q, d).wait_send()
                stage3(s, q, d).wait_send()
    for c in outs:
        c.wait()


def per_device(
    n, tiles,
    ensemble, control, weights, member_band, spread, advect, damping, innovation, obs_weight
):
    ml, vl, rows, ny = ensemble.shape
    assert rows == SWEEPS and ny % 128 == 0 and ml <= 8 and vl % (2 * n) == 0
    steps = max(d for d in range(1, STEPS + 1) if (vl // (2 * n)) % d == 0)
    planes = vl // (2 * n * steps)
    a, b = factors(n)
    f32 = jnp.float32
    peers = max(a, b, 2) - 1
    dma = pltpu.SemaphoreType.DMA
    hbm = pl.BlockSpec(memory_space=pl.ANY)
    field = (rows, ny)
    out, gw = pl.pallas_call(
        functools.partial(kernel, n, tiles, steps, planes),
        out_shape=(
            jax.ShapeDtypeStruct((ml, rows, ny), f32),
            jax.ShapeDtypeStruct((8, 128), f32),
        ),
        in_specs=[hbm] * 9,
        out_specs=(hbm, hbm),
        scratch_shapes=[
            pltpu.VMEM(control.shape, f32),
            pltpu.SMEM(weights.shape, f32),
            pltpu.SMEM(member_band.shape, member_band.dtype),
            pltpu.SMEM(spread.shape, f32),
            pltpu.SMEM(advect.shape, f32),
            pltpu.SMEM(damping.shape, f32),
            pltpu.VMEM(obs_weight.shape, f32),
            pltpu.VMEM(control.shape, f32),
            pltpu.VMEM((8, 128), f32),
            dma((7,)),
            dma((2,)),
            pltpu.VMEM((ml, vl) + field, ensemble.dtype),
            pltpu.VMEM((steps * 2 * planes,) + field, f32),
            pltpu.VMEM((ml,) + field, f32),
            pltpu.VMEM((ml,) + field, f32),
            pltpu.VMEM((ml,) + field, f32),
            pltpu.VMEM((steps, 2 * planes) + field, f32),
            pltpu.VMEM((steps, 2, n * planes) + field, f32),
            pltpu.VMEM((steps, 2, n * planes) + field, f32),
            pltpu.VMEM((steps, max(b - 1, 1), a * planes) + field, f32),
            pltpu.VMEM((steps, max(a - 1, 1), b * planes) + field, f32),
            pltpu.VMEM((steps, max(a - 1, 1), planes) + field, f32),
            pltpu.VMEM((steps, max(b - 1, 1), planes) + field, f32),
            pltpu.VMEM((2, ml) + field, f32),
            pltpu.VMEM((2,) + field, f32),
            pltpu.VMEM((2, steps * 2 * planes) + field, f32),
            pltpu.VMEM((2, steps, 2 * planes) + field, f32),
            pltpu.VMEM((2, ml) + field, f32),
            pltpu.VMEM((tiles, 8, 128), f32),
            dma((ml,)),
            dma((steps, 2)),
        ]
        + [dma((steps, 2, peers))] * 8
        + [dma((2, steps))] * 2
        + [dma((8,))] * 2
        + [dma((tiles - 1,))] * 2,
        compiler_params=pltpu.CompilerParams(
            collective_id=0, has_side_effects=True, vmem_limit_bytes=63 * 1024 * 1024
        ),
    )(ensemble, control, weights, member_band, spread, advect, damping, innovation, obs_weight)
    total_cells = tiles * rows * ny * vl
    return out, gw[:ml, 0] / math.sqrt(total_cells)


def solution(mesh):
    in_specs = (
        P("mem", None, "tile", None),
        P("mem", "tile", None),
        P("mem"),
        P("mem"),
        P(),
        P(),
        P(),
        P(None, "tile", None),
        P("tile", None),
    )
    out_specs = (P("mem", "tile", None), P("mem"))
    return jax.shard_map(
        functools.partial(per_device, mesh.shape["mem"], mesh.shape["tile"]),
        mesh=mesh, in_specs=in_specs, out_specs=out_specs, check_vma=False,
    )
```
